32 devices in a mesh: cube: 2 (over y), facet: 4 (over z), chan: 2 (over x), sub: 2 (over core).
Axes of the slice: x: 2, y: 2, z: 4, core: 2. Of those that a mesh axis runs over, the one named last changes fastest.
Arguments:
- image: float32 [128, 256, 512], P(('cube', 'chan'), ('facet', 'sub')), parts along dimension 0, may hold values from 0 to 2
- dual_nuclear: float32 [128, 256, 512], P(('cube', 'chan'), ('facet', 'sub')), parts along dimension 0, may hold values from -25 to 25
- dual_wavelet: bfloat16 [128, 4, 256, 512], P(('cube', 'chan'), None, ('facet', 'sub')), parts along dimension 0, may hold values from -3 to 3
- dual_data: float32 [128, 2, 512, 128], P(('cube', 'chan'), None, ('facet', 'sub')), parts along dimension 0, may hold values from -3 to 3
- observed: float32 [128, 2, 512, 128], P(('cube', 'chan'), None, ('facet', 'sub')), parts along dimension 0, may hold values from -6 to 6
- sample_rows: int32 [128, 128], P(('cube', 'chan')), parts along dimension 0, may hold values from 0 to 255
Outputs:
- image_next: float32 [128, 256, 512], P(('cube', 'chan'), ('facet', 'sub')), parts along dimension 0
- nuclear_next: float32 [128, 256, 512], P(('cube', 'chan'), ('facet', 'sub')), parts along dimension 0
- wavelet_next: bfloat16 [128, 4, 256, 512], P(('cube', 'chan'), None, ('facet', 'sub')), parts along dimension 0
- data_next: float32 [128, 2, 512, 128], P(('cube', 'chan'), None, ('facet', 'sub')), parts along dimension 0
The draws below stay inside these ranges and needn't reach their ends.
There are 2 independent parts, one for each index of `cube`. The reference program is written for one: setup_inputs(seed, part) draws one part's arguments, and reference() takes and returns one part's arrays. A program takes and returns all parts, laid end to end along the dimension named above; each array names one. Nothing has to cross between parts.
Inputs may be any that keep to these rules, and one draw needn't show every extreme that they name: `sample_rows`: indices may repeat within a channel.
All inputs are finite; a program needn't handle non-finite values.
Results may differ from the reference program's by a relative error of at most 0.0083.
Values may be sent and summed in bfloat16 or wider, within the bound.
No kernel may reach another device: no remote copies, remote signals or barrier semaphores. Data moves between devices by JAX's collectives and lax.ppermute only.
A program may use at most 128 MiB of HBM per device.

```python
import math
import jax
import jax.numpy as jnp
from jax import lax

CH = 64
NX = 512
SAMPLES = 128
NS_STEPS = 6
NY = 256
FACET_PIX = 32768
N_FACET = 4


def draw_dual_nuclear(key, part):
    key_scale, key_noise = jax.random.split(key, 2)
    scales = jnp.exp(jax.random.uniform(key_scale, (CH, 1, 1), jnp.float32, 0.0, jnp.log(10.0)))
    noise = jnp.clip(jax.random.normal(key_noise, (CH, NY, NX), jnp.float32), -4.0, 4.0)
    result = 0.3 * scales * noise
    return result


def plant(entries, own_key, smallest, high):
    place = [jax.random.randint(jax.random.fold_in(own_key, axis), (), 0, length) for axis, length in enumerate(entries.shape)]
    widest = entries.shape.index(max(entries.shape))
    next_to = place[:widest] + [(place[widest] + 1) % entries.shape[widest]] + place[widest + 1:]
    return entries.at[tuple(place)].set(smallest).at[tuple(next_to)].set(high)


def steps_of(stream_key, dims, cuts, low, high):
    def one(axis_at, shards_of):
        heights = jax.random.uniform(jax.random.fold_in(jax.random.fold_in(stream_key, 6), axis_at), (shards_of,), jnp.float32, low / len(cuts), high / len(cuts))
        return jnp.repeat(jnp.exp(heights), dims[axis_at] // shards_of).reshape((-1,) + (1,) * (len(dims) - axis_at - 1))

    factor_of = one(*cuts[0])
    for cut in cuts[1:]:
        factor_of = factor_of * one(*cut)
    return factor_of


def scatter_about(own_key, shape, spread, most, cuts=(), kind=jnp.bfloat16):
    drawn = spread * jax.random.normal(own_key, shape, jnp.float32)
    if cuts:
        drawn = drawn * steps_of(own_key, shape, cuts, -0.22, 0.18)
    return jnp.clip(drawn, -most, most).astype(kind)


def setup_inputs(seed: int = 0, part: int = 0) -> dict:
    streams_of = jax.random.split(jax.random.key(seed), 7)
    part_splits = jax.random.split(jax.random.fold_in(streams_of[6], part), 7)
    image = jnp.clip(2.0 * jax.random.uniform(part_splits[0], (CH, NY, NX), jnp.float32) ** steps_of(part_splits[0], (CH, NY, NX), ((0, 2), (1, 8)), -0.2, 0.2), 0.0, 2.0)
    dual_nuclear = draw_dual_nuclear(jax.random.fold_in(jax.random.fold_in(streams_of[6], part), 71), part)
    dual_wavelet = scatter_about(part_splits[2], (CH, 4, NY, NX), 0.5, 3.0, ((0, 2), (2, 8)))
    dual_data = scatter_about(part_splits[3], (CH, 2, NX, SAMPLES), 0.5, 3.0, ((0, 2), (2, 8)), jnp.float32)
    observed = scatter_about(part_splits[4], (CH, 2, NX, SAMPLES), 1.0, 6.0, ((0, 2), (2, 8)), jnp.float32)
    sample_rows = plant(jax.random.randint(part_splits[5], (CH, SAMPLES), 0, NY), jax.random.fold_in(part_splits[5], 1), 0, NY - 1).astype(jnp.int32)
    return {"image": image, "dual_nuclear": dual_nuclear, "dual_wavelet": dual_wavelet, "dual_data": dual_data, "observed": observed, "sample_rows": sample_rows}


LOWPASS = [0.48296291314453416, 0.8365163037378079, 0.2241438680420134, -0.12940952255126037]
FILTERS = [[value / math.sqrt(2.0) for value in LOWPASS], [(-1.0) ** index * LOWPASS[3 - index] / math.sqrt(2.0) for index in range(4)]]
HIGH = lax.Precision.HIGHEST

def filter_last(values, taps, adjoint):
    length = values.shape[-1]
    widths = [(0, 0)] * (values.ndim - 1) + [(2, 1) if adjoint else (1, 2)]
    padded = jnp.pad(values, widths)
    if adjoint:
        return sum((taps[index] * padded[..., 3 - index:3 - index + length] for index in range(4)))
    return sum((taps[index] * padded[..., index:index + length] for index in range(4)))

def filter_rows(values, taps, adjoint):
    return jnp.swapaxes(filter_last(jnp.swapaxes(values, -1, -2), taps, adjoint), -1, -2)

def analysis(field):
    bands = []
    for row_band in range(2):
        rowed = filter_rows(field, FILTERS[row_band], False)
        for col_band in range(2):
            bands.append(filter_last(rowed, FILTERS[col_band], False))
    return jnp.stack(bands, 1)

def synthesis(bands):
    total = 0.0
    for row_band in range(2):
        colled = sum((filter_last(bands[:, 2 * row_band + col_band], FILTERS[col_band], True) for col_band in range(2)))
        total = total + filter_rows(colled, FILTERS[row_band], True)
    return total

def lowered(values):
    return lax.optimization_barrier(values.astype(jnp.bfloat16)).astype(jnp.float32)

def phase_tables(freqs, places, period):
    product = freqs.astype(jnp.int32)[..., None] * places.astype(jnp.int32) % period
    angles = 2.0 * math.pi / period * product.astype(jnp.float32)
    norm = 1.0 / math.sqrt(period)
    return (lowered(jnp.cos(angles) * norm), lowered(jnp.sin(angles) * norm))

def reference(image, dual_nuclear, dual_wavelet, dual_data, observed, sample_rows):
    col_places = jnp.arange(NX, dtype=jnp.int32)
    row_places = jnp.arange(NY, dtype=jnp.int32)
    col_cos, col_sin = phase_tables(col_places, col_places, NX)
    row_cos, row_sin = phase_tables(sample_rows, row_places, NY)
    dual_real = lowered(dual_data[:, 0])
    dual_imag = lowered(dual_data[:, 1])
    spread_real = jnp.einsum('cky,cqk->cyq', row_cos, dual_real, precision=HIGH) - jnp.einsum('cky,cqk->cyq', row_sin, dual_imag, precision=HIGH)
    spread_imag = jnp.einsum('cky,cqk->cyq', row_cos, dual_imag, precision=HIGH) + jnp.einsum('cky,cqk->cyq', row_sin, dual_real, precision=HIGH)
    spread_real = lowered(spread_real)
    spread_imag = lowered(spread_imag)
    back_data = jnp.einsum('cyq,qx->cyx', spread_real, col_cos, precision=HIGH) - jnp.einsum('cyq,qx->cyx', spread_imag, col_sin, precision=HIGH)
    wave_float = dual_wavelet.astype(jnp.float32)
    back = back_data + synthesis(wave_float)
    image_next = jnp.maximum(image - 0.5 * (back + dual_nuclear), 0.0)
    field = 2.0 * image_next - image
    field_low = lowered(field)
    spec_real = lowered(jnp.einsum('cyx,xq->cyq', field_low, col_cos, precision=HIGH))
    spec_imag = lowered(-jnp.einsum('cyx,xq->cyq', field_low, col_sin, precision=HIGH))
    samp_real = jnp.einsum('cky,cyq->cqk', row_cos, spec_real, precision=HIGH) + jnp.einsum('cky,cyq->cqk', row_sin, spec_imag, precision=HIGH)
    samp_imag = jnp.einsum('cky,cyq->cqk', row_cos, spec_imag, precision=HIGH) - jnp.einsum('cky,cyq->cqk', row_sin, spec_real, precision=HIGH)
    sampled = jnp.stack([samp_real, samp_imag], 1)
    data_next = (dual_data + 0.5 * (sampled - observed)) / 1.5
    bands = wave_float + 0.5 * analysis(field)
    power = lax.optimization_barrier(jnp.sum(bands * bands, 0))
    limit = 0.6 * math.sqrt(CH)
    wavelet_next = (bands / jnp.maximum(1.0, jnp.sqrt(power) / limit)).astype(jnp.bfloat16)
    stacked = (dual_nuclear + field).astype(jnp.bfloat16)
    facets = stacked.reshape(CH, N_FACET, -1).transpose(1, 0, 2).astype(jnp.float32)
    gram = jnp.einsum('fcp,fdp->fcd', facets, facets, precision=HIGH)
    trace_sum = jnp.trace(gram, axis1=1, axis2=2)
    approx = (2.0 / trace_sum)[:, None, None] * gram
    eye_mat = jnp.broadcast_to(jnp.eye(CH, dtype=jnp.float32), gram.shape)
    root = eye_mat
    for turn in range(NS_STEPS):
        newton = 1.5 * eye_mat - 0.5 * jnp.einsum('fij,fjk->fik', root, approx, precision=HIGH)
        approx = jnp.einsum('fij,fjk->fik', approx, newton, precision=HIGH)
        root = jnp.einsum('fij,fjk->fik', newton, root, precision=HIGH)
    root_low = lowered(root)
    mixed = jnp.einsum('fcd,fdp->fcp', root_low, facets, precision=HIGH)
    mixed = mixed * jnp.sqrt(2.0 * FACET_PIX / trace_sum)[:, None, None]
    nuclear_next = mixed.transpose(1, 0, 2).reshape(CH, NY, NX)
    return (image_next, nuclear_next, wavelet_next, data_next)
```

```python
import functools
import math

import jax
import jax.numpy as jnp
import numpy as np
from jax import lax
from jax.experimental import pallas as pl
from jax.experimental.pallas import tpu as pltpu
from jax.sharding import PartitionSpec as P

CH = 64
NS_STEPS = 6


LOWPASS = [0.48296291314453416, 0.8365163037378079, 0.2241438680420134, -0.12940952255126037]
FILTERS = [
    [value / math.sqrt(2.0) for value in LOWPASS],
    [(-1.0) ** index * LOWPASS[3 - index] / math.sqrt(2.0) for index in range(4)],
]
HIGH = lax.Precision.HIGHEST
LOW = jnp.bfloat16
F32 = jnp.float32
LINE = ("facet", "sub")
MIB = 1 << 20


def host_tables(period):
    index = np.arange(period)
    product = np.outer(index, index) % period
    angles = np.float32(2.0 * math.pi / period) * product.astype(np.float32)
    norm = np.float32(1.0 / math.sqrt(period))
    cos = (np.cos(angles).astype(np.float32) * norm).astype(LOW)
    sin = (np.sin(angles).astype(np.float32) * norm).astype(LOW)
    return cos, sin


def position():
    return lax.axis_index("facet") * lax.axis_size("sub") + lax.axis_index("sub")


def pick(channels, most):
    size = most
    while channels % size:
        size //= 2
    return size


def params(limit=None):
    return pltpu.CompilerParams(
        dimension_semantics=("arbitrary",), vmem_limit_bytes=limit
    )


def whole_spec(array):
    return pl.BlockSpec(array.shape, lambda i: (0,) * array.ndim)


def chan_spec(array, size):
    return pl.BlockSpec(
        (size,) + array.shape[1:], lambda i: (i,) + (0,) * (array.ndim - 1)
    )


def spread_kernel(n, size, rows_ref, base_ref, dual_ref, table_ref, *rest):
    outs, hold = rest[:n], rest[n]
    me = position()
    height = table_ref.shape[1]
    samples = rows_ref.shape[1]
    width = dual_ref.shape[2]
    step = pl.program_id(0)
    group = 2 if size % 2 == 0 else 1
    for first in range(0, size, group):
        index = [rows_ref[pl.ds(step * size + first + i, 1), :] for i in range(group)]
        index = jnp.concatenate(index, axis=1) if group > 1 else index[0]
        places = lax.broadcasted_iota(jnp.int32, (height, group * samples), 0)
        hot = jnp.where(places == index, 1.0, 0.0).astype(LOW)
        both = jnp.dot(base_ref[...], hot, preferred_element_type=F32).astype(LOW)
        for i in range(group):
            c = first + i
            columns = slice(i * samples, (i + 1) * samples)
            table = jnp.concatenate([both[:height, columns], both[height:, columns]], axis=1)
            table_ref[c] = table
            real, imag = dual_ref[c, 0], dual_ref[c, 1]
            right = jnp.concatenate(
                [
                    jnp.concatenate([real, -imag], axis=1),
                    jnp.concatenate([imag, real], axis=1),
                ],
                axis=0,
            ).astype(LOW)
            spread = lax.dot_general(
                table, right, (((1,), (1,)), ((), ())), preferred_element_type=F32
            ).astype(LOW)
            hold[c] = spread.reshape(n, height // n, 2 * width)
            for d in range(n):
                outs[d][c] = hold[c, lax.rem(me + d, n)]


def spread_call(n, height, sample_rows, row_base, dual_data):
    channels, _, width, samples = dual_data.shape
    size = pick(channels, 4)
    block = jax.ShapeDtypeStruct((channels, height // n, 2 * width), LOW)
    table = jax.ShapeDtypeStruct((channels, height, 2 * samples), LOW)
    return pl.pallas_call(
        functools.partial(spread_kernel, n, size),
        grid=(channels // size,),
        out_shape=(table,) + (block,) * n,
        in_specs=[whole_spec(sample_rows), whole_spec(row_base), chan_spec(dual_data, size)],
        out_specs=(chan_spec(table, size),) + (chan_spec(block, size),) * n,
        scratch_shapes=[pltpu.VMEM((size, n, height // n, 2 * width), LOW)],
        compiler_params=params(),
        name="spread",
        cost_estimate=pl.CostEstimate(
            flops=6 * 10**9, bytes_accessed=10 * 10**6, transcendentals=0
        ),
    )(sample_rows, row_base, dual_data)


def synth_kernel(size, wave_ref, before_ref, after_ref, image_ref, dual_ref, out_ref, hold):
    rows, columns = image_ref.shape[1:]
    lane = lax.broadcasted_iota(jnp.int32, (rows, columns), 1)

    def one(c, _):
        for band in range(4):
            hold[band, 8 : 8 + rows] = wave_ref[c, band].astype(F32)
            hold[band, 6:8] = before_ref[c, band].astype(F32)
            hold[band, 8 + rows : 9 + rows] = after_ref[c, band].astype(F32)
        mixed = []
        for col_band in range(2):
            total = None
            for row_band in range(2):
                for k in range(4):
                    term = FILTERS[row_band][k] * hold[2 * row_band + col_band, pl.ds(9 - k, rows)]
                    total = term if total is None else total + term
            mixed.append(total)
        synth = FILTERS[0][1] * mixed[0] + FILTERS[1][1] * mixed[1]
        for k in (0, 2, 3):
            part = FILTERS[0][k] * mixed[0] + FILTERS[1][k] * mixed[1]
            part = pltpu.roll(part, (k - 1) % columns, 1)
            inside = lane < columns - 1 if k == 0 else lane >= k - 1
            synth = synth + jnp.where(inside, part, 0.0)
        out_ref[c] = image_ref[c] - 0.5 * (synth + dual_ref[c])
        return 0

    lax.fori_loop(0, size, one, 0)


def synth_call(wave, before, after, image, dual_nuclear):
    channels, rows, columns = image.shape
    size = pick(channels, 4)
    args = (wave, before, after, image, dual_nuclear)
    return pl.pallas_call(
        functools.partial(synth_kernel, size),
        grid=(channels // size,),
        out_shape=jax.ShapeDtypeStruct(image.shape, F32),
        in_specs=[chan_spec(a, size) for a in args],
        out_specs=chan_spec(image, size),
        scratch_shapes=[pltpu.VMEM((4, rows + 16, columns), F32)],
        compiler_params=params(),
        name="synth",
        cost_estimate=pl.CostEstimate(
            flops=6 * 10**9, bytes_accessed=10 * 10**6, transcendentals=0
        ),
    )(*args)


def image_kernel(n, size, *refs):
    got, (col_ref, base_ref, image_ref, dual_ref) = refs[:n], refs[n : n + 4]
    next_ref, stacked_ref, top_ref, bottom_ref = refs[n + 4 : n + 8]
    outs = refs[n + 8 :]
    me = position()
    rows, columns = image_ref.shape[1:]
    width = got[0].shape[2]
    tall = size * rows
    blocks = [got[d][...].reshape(tall, width) for d in range(n)]
    back_tables = [col_ref[lax.rem(me + n - d, n)] for d in range(n)]
    if width % 128 == 0:
        back = jnp.dot(
            jnp.concatenate(blocks, axis=1),
            jnp.concatenate(back_tables, axis=0),
            preferred_element_type=F32,
        )
    else:
        back = sum(
            jnp.dot(block, table, preferred_element_type=F32)
            for block, table in zip(blocks, back_tables)
        )
    image = image_ref[...].reshape(tall, columns)
    following = jnp.maximum(base_ref[...].reshape(tall, columns) - 0.5 * back, 0.0)
    next_ref[...] = following.reshape(size, rows, columns)
    field = 2.0 * following - image
    stacked_ref[...] = (dual_ref[...].reshape(tall, columns) + field).astype(LOW).reshape(
        size, rows, columns
    )
    low = field.astype(LOW)
    edges = field.reshape(size, rows, columns)
    top_ref[...] = edges[:, 0:2].astype(LOW)
    bottom_ref[...] = edges[:, rows - 1 : rows].astype(LOW)
    forward = [col_ref[lax.rem(me + d, n)] for d in range(n)]
    form = (((1,), (1,)), ((), ()))
    if width % 128 == 0:
        spectra = lax.dot_general(
            low, jnp.concatenate(forward, axis=0), form, preferred_element_type=F32
        ).astype(LOW)
        parts = [spectra[:, d * width : (d + 1) * width] for d in range(n)]
    else:
        parts = [
            lax.dot_general(low, table, form, preferred_element_type=F32).astype(LOW)
            for table in forward
        ]
    for d in range(n):
        outs[d][...] = parts[d].reshape(size, rows, width)


def image_call(n, got, col_table, base, image, dual_nuclear):
    channels, rows, columns = image.shape
    size = pick(channels, 8)
    edge = lambda count: jax.ShapeDtypeStruct((channels, count, columns), LOW)
    outs = (
        jax.ShapeDtypeStruct(image.shape, F32),
        jax.ShapeDtypeStruct(image.shape, LOW),
        edge(2),
        edge(1),
    ) + tuple(jax.ShapeDtypeStruct(g.shape, LOW) for g in got)
    return pl.pallas_call(
        functools.partial(image_kernel, n, size),
        grid=(channels // size,),
        out_shape=outs,
        in_specs=[chan_spec(g, size) for g in got]
        + [whole_spec(col_table)]
        + [chan_spec(a, size) for a in (base, image, dual_nuclear)],
        out_specs=tuple(chan_spec(o, size) for o in outs),
        compiler_params=params(),
        name="image",
        cost_estimate=pl.CostEstimate(
            flops=6 * 10**9, bytes_accessed=10 * 10**6, transcendentals=0
        ),
    )(*got, col_table, base, image, dual_nuclear)


def sample_kernel(n, size, *refs):
    got, (table_ref, dual_ref, seen_ref, out_ref, hold) = refs[:n], refs[n:]
    me = position()
    height, pairs = table_ref.shape[1:]
    samples = pairs // 2
    width = dual_ref.shape[2]
    for c in range(size):
        for d in range(n):
            hold[c, lax.rem(me + n - d, n)] = got[d][c]
        product = lax.dot_general(
            hold[c].reshape(height, 2 * width),
            table_ref[c],
            (((0,), (0,)), ((), ())),
            preferred_element_type=F32,
        )
        real = product[:width, :samples] + product[width:, samples:]
        imag = product[width:, :samples] - product[:width, samples:]
        for part, value in ((0, real), (1, imag)):
            out_ref[c, part] = (dual_ref[c, part] + 0.5 * (value - seen_ref[c, part])) / 1.5


def sample_call(n, got, table, dual_data, observed):
    channels, _, width, _ = dual_data.shape
    height = table.shape[1]
    size = pick(channels, 4)
    args = tuple(got) + (table, dual_data, observed)
    return pl.pallas_call(
        functools.partial(sample_kernel, n, size),
        grid=(channels // size,),
        out_shape=jax.ShapeDtypeStruct(dual_data.shape, F32),
        in_specs=[chan_spec(a, size) for a in args],
        out_specs=chan_spec(dual_data, size),
        scratch_shapes=[pltpu.VMEM((size, n, height // n, 2 * width), LOW)],
        compiler_params=params(),
        name="sample",
        cost_estimate=pl.CostEstimate(
            flops=6 * 10**9, bytes_accessed=10 * 10**6, transcendentals=0
        ),
    )(*args)


def bands_kernel(size, final, *refs):
    next_ref, image_ref, wave_ref, before_ref, after_ref = refs[:5]
    if final:
        power_ref, out_ref, wide, filtered, scale = refs[5:]
    else:
        out_ref, wide, filtered, scale = refs[5:]
    rows, columns = image_ref.shape[1:]
    tall = rows + 16
    lane = lax.broadcasted_iota(jnp.int32, (tall, columns), 1)

    @pl.when(pl.program_id(0) == 0)
    def _():
        wide[...] = jnp.zeros_like(wide)
        if final:
            limit = 0.6 * math.sqrt(CH)
            scale[...] = 1.0 / jnp.maximum(1.0, jnp.sqrt(power_ref[...]) / limit)
        else:
            scale[...] = jnp.zeros_like(scale)

    def one(c, _):
        wide[8 : 8 + rows] = 2.0 * next_ref[c] - image_ref[c]
        wide[7:8] = before_ref[c].astype(F32)
        wide[8 + rows : 10 + rows] = after_ref[c].astype(F32)
        field = wide[...]
        shifted = [
            jnp.where(lane >= 1, pltpu.roll(field, 1, 1), 0.0),
            field,
            jnp.where(lane < columns - 1, pltpu.roll(field, columns - 1, 1), 0.0),
            jnp.where(lane < columns - 2, pltpu.roll(field, columns - 2, 1), 0.0),
        ]
        for col_band in range(2):
            taps = FILTERS[col_band]
            filtered[col_band] = sum(taps[k] * shifted[k] for k in range(4))
        for row_band in range(2):
            taps = FILTERS[row_band]
            for col_band in range(2):
                band = 2 * row_band + col_band
                value = sum(
                    0.5 * taps[k] * filtered[col_band, pl.ds(7 + k, rows)] for k in range(4)
                )
                value = wave_ref[c, band].astype(F32) + value
                if final:
                    out_ref[c, band] = (value * scale[band]).astype(LOW)
                else:
                    scale[band] += value * value
        return 0

    lax.fori_loop(0, size, one, 0)
    if not final:

        @pl.when(pl.program_id(0) == pl.num_programs(0) - 1)
        def _():
            out_ref[...] = scale[...].astype(LOW)


def bands_call(following, image, wave, before, after, power=None):
    channels, rows, columns = image.shape
    size = pick(channels, 4)
    args = (following, image, wave, before, after)
    specs = [chan_spec(a, size) for a in args]
    final = power is not None
    if final:
        args += (power,)
        specs += [whole_spec(power)]
        out = jax.ShapeDtypeStruct(wave.shape, LOW)
        out_spec = chan_spec(out, size)
    else:
        out = jax.ShapeDtypeStruct((4, rows, columns), LOW)
        out_spec = whole_spec(out)
    return pl.pallas_call(
        functools.partial(bands_kernel, size, final),
        grid=(channels // size,),
        out_shape=out,
        in_specs=specs,
        out_specs=out_spec,
        scratch_shapes=[
            pltpu.VMEM((rows + 16, columns), F32),
            pltpu.VMEM((2, rows + 16, columns), F32),
            pltpu.VMEM((4, rows, columns), F32),
        ],
        compiler_params=params(),
        name="result" if final else "power",
        cost_estimate=pl.CostEstimate(
            flops=4 * 10**9, bytes_accessed=10 * 10**6, transcendentals=0
        ),
    )(*args)


def polar_mixing(gram, pixels):
    trace_sum = jnp.trace(gram)
    approx = 2.0 / trace_sum * gram
    eye_mat = jnp.eye(gram.shape[0], dtype=jnp.float32)
    root = eye_mat
    for turn in range(NS_STEPS):
        newton = 1.5 * eye_mat - 0.5 * jnp.dot(root, approx, precision=HIGH)
        approx = jnp.dot(approx, newton, precision=HIGH)
        root = jnp.dot(newton, root, precision=HIGH)
    return (root.astype(LOW), jnp.sqrt(2.0 * pixels / trace_sum))


def rotated(values, axis, shift):
    count = lax.axis_size(axis)
    return lax.ppermute(values, axis, [(i, (i + shift) % count) for i in range(count)])


def far_first(n):
    return sorted(range(1, n), key=lambda d: abs(d - n / 2))


def exchanged(blocks):
    n = len(blocks)
    got = list(blocks)
    for d in far_first(n):
        got[d] = rotated(blocks[d], LINE, d)
    return got


def neighbours(first, last):
    count = lax.axis_size(LINE)
    up = [(i, i + 1) for i in range(count - 1)]
    down = [(j, i) for i, j in up]
    return lax.ppermute(last, LINE, up), lax.ppermute(first, LINE, down)


def total(values, axis):
    result = values.astype(F32)
    for d in range(1, lax.axis_size(axis)):
        result = result + rotated(values, axis, d).astype(F32)
    return result


def shards(image, dual_nuclear, dual_wavelet, dual_data, observed, sample_rows):
    channels, row_count, columns = image.shape
    halves = lax.axis_size("sub")
    n = lax.axis_size("facet") * halves
    height = row_count * n
    width = columns // n
    row_base = jnp.asarray(np.concatenate(host_tables(height), axis=0))
    col_cos, col_sin = host_tables(columns)
    col_table = jnp.asarray(
        np.concatenate(
            [
                col_cos.reshape(n, width, columns),
                (-col_sin.astype(np.float32)).astype(LOW).reshape(n, width, columns),
            ],
            axis=1,
        )
    )

    wave_before, wave_after = neighbours(
        dual_wavelet[:, :, :1], dual_wavelet[:, :, row_count - 2 :]
    )
    table, *spread = spread_call(n, height, sample_rows, row_base, dual_data)
    pieces = exchanged(spread)
    base = synth_call(dual_wavelet, wave_before, wave_after, image, dual_nuclear)
    image_next, stacked, top, bottom, *spectra = image_call(
        n, pieces, col_table, base, image, dual_nuclear
    )
    gathered = exchanged(spectra)

    z_before, z_after = neighbours(top, bottom)
    stacked = stacked.reshape(channels, -1)
    whole = [stacked] + [
        rotated(stacked, "chan", d) for d in range(1, lax.axis_size("chan"))
    ]
    power = bands_call(image_next, image, dual_wavelet, z_before, z_after)
    power = total(power, "chan")
    wavelet_next = bands_call(image_next, image, dual_wavelet, z_before, z_after, power)

    whole = jnp.concatenate(whole, axis=0)
    gram = jnp.dot(whole, whole.T, preferred_element_type=F32)
    gram = total(gram, "sub")
    mixing, factor = polar_mixing(gram, row_count * columns * halves)
    nuclear_next = factor * jnp.dot(mixing[:channels], whole, preferred_element_type=F32)
    nuclear_next = nuclear_next.reshape(channels, row_count, columns)

    data_next = sample_call(n, gathered, table, dual_data, observed)
    return (image_next, nuclear_next, wavelet_next, data_next)


def solution(mesh):
    placed = (
        P(("cube", "chan"), ("facet", "sub"), None),
        P(("cube", "chan"), ("facet", "sub"), None),
        P(("cube", "chan"), None, ("facet", "sub"), None),
        P(("cube", "chan"), None, ("facet", "sub"), None),
        P(("cube", "chan"), None, ("facet", "sub"), None),
        P(("cube", "chan"), None),
    )
    return jax.shard_map(
        shards,
        mesh=mesh,
        in_specs=placed,
        out_specs=(
            P(("cube", "chan"), ("facet", "sub"), None),
            P(("cube", "chan"), ("facet", "sub"), None),
            P(("cube", "chan"), None, ("facet", "sub"), None),
            P(("cube", "chan"), None, ("facet", "sub"), None),
        ),
        check_vma=False,
    )
```

```python
import functools
import math

import jax
import jax.numpy as jnp
import numpy as np
from jax import lax
from jax.experimental import pallas as pl
from jax.experimental.pallas import tpu as pltpu
from jax.sharding import PartitionSpec as P


CH = 64
NS_STEPS = 6


LOWPASS = [0.48296291314453416, 0.8365163037378079, 0.2241438680420134, -0.12940952255126037]
HIGH = lax.Precision.HIGHEST
LOW = jnp.bfloat16
F32 = jnp.float32
LINE = ("facet", "sub")
MIB = 1 << 20


def host_tables(period):
    index = np.arange(period)
    product = np.outer(index, index) % period
    angles = np.float32(2.0 * math.pi / period) * product.astype(np.float32)
    norm = np.float32(1.0 / math.sqrt(period))
    cos = (np.cos(angles).astype(np.float32) * norm).astype(LOW)
    sin = (np.sin(angles).astype(np.float32) * norm).astype(LOW)
    return cos, sin


def position():
    return lax.axis_index("facet") * lax.axis_size("sub") + lax.axis_index("sub")


def partner(me, d, n):
    assert n & (n - 1) == 0
    return me ^ d


def pick(channels, most):
    size = most
    while channels % size:
        size //= 2
    return size


def nbytes(array):
    return math.prod(array.shape) * jnp.dtype(array.dtype).itemsize


def streamed(body, ins, whole, outs, chunks, scratch=(), earlier=(), late=None, soon=(), room=True):
    counts = [a.shape[0] // chunks for a in ins], [a.shape[0] // chunks for a in outs]

    def kernel(*refs):
        refs = list(refs)
        take = lambda count: [refs.pop(0) for _ in range(count)]
        in_far, whole_near, _ = take(len(ins)), take(len(whole)), take(len(earlier))
        soon_far = take(len(soon))
        out_far, in_near, out_near = take(len(outs)), take(len(ins)), take(len(outs))
        extra, soon_near = take(len(scratch)), take(len(soon))
        in_sem, out_sem, soon_sem = refs
        firsts = [
            pltpu.make_async_copy(soon_far[a], soon_near[a], soon_sem.at[a])
            for a in range(len(soon))
        ]

        def arrival(a, i):
            part = pl.ds(i * counts[0][a], counts[0][a])
            return pltpu.make_async_copy(
                in_far[a].at[part], in_near[a].at[part], in_sem.at[a, i]
            )

        def departure(a, i):
            part = pl.ds(i * counts[1][a], counts[1][a])
            return pltpu.make_async_copy(
                out_near[a].at[part], out_far[a].at[part], out_sem.at[a, i]
            )

        for copy in firsts:
            copy.start()

        @pl.loop(0, chunks)
        def _(i):
            for a in range(len(ins)):
                arrival(a, i).start()

        for copy in firsts:
            copy.wait()

        @pl.loop(0, chunks)
        def _(i):
            for a in range(len(ins)):
                arrival(a, i).wait()
            body(i, in_near, whole_near + soon_near, out_near, extra)
            if late is None:
                for a in range(len(outs)):
                    departure(a, i).start()

        if late is None:

            @pl.loop(0, chunks)
            def _(i):
                for a in range(len(outs)):
                    departure(a, i).wait()

        else:
            late(out_near, extra)
            for a in range(len(outs)):
                copy = pltpu.make_async_copy(out_near[a], out_far[a], out_sem.at[a, 0])
                copy.start()
                copy.wait()

    far = pl.BlockSpec(memory_space=pltpu.HBM)
    anywhere = pl.BlockSpec(memory_space=pl.ANY)
    near = pl.BlockSpec(memory_space=pltpu.VMEM)
    moved_bytes = sum(nbytes(a) for a in list(ins) + list(outs) + list(whole))
    return pl.pallas_call(
        kernel,
        out_shape=tuple(outs),
        in_specs=[far] * len(ins)
        + [near] * len(whole)
        + [anywhere] * len(earlier)
        + [far] * len(soon),
        out_specs=(far,) * len(outs),
        scratch_shapes=[pltpu.VMEM(a.shape, a.dtype) for a in list(ins) + list(outs)]
        + list(scratch)
        + [pltpu.VMEM(a.shape, a.dtype) for a in soon]
        + [
            pltpu.SemaphoreType.DMA((max(len(ins), 1), chunks)),
            pltpu.SemaphoreType.DMA((len(outs), chunks)),
            pltpu.SemaphoreType.DMA((max(len(soon), 1),)),
        ],
        compiler_params=pltpu.CompilerParams(
            vmem_limit_bytes=sum(nbytes(a) for a in list(ins) + list(outs)) + 14 * MIB
            if room
            else None
        ),
        cost_estimate=pl.CostEstimate(
            flops=4 * 10**9, bytes_accessed=moved_bytes, transcendentals=0
        ),
    )(*ins, *whole, *earlier, *soon)


def shape_of(shape, dtype):
    return jax.ShapeDtypeStruct(shape, dtype)


def spread_body(n, size, i, ins, whole, outs, scratch):
    (dual_ref,), (rows_ref, base_ref), (table_ref, *outs), (hold,) = ins, whole, outs, scratch
    me = position()
    height = table_ref.shape[1]
    samples = rows_ref.shape[1]
    width = dual_ref.shape[2]
    group = 2 if size % 2 == 0 else 1
    for first in range(0, size, group):
        index = [rows_ref[pl.ds(i * size + first + j, 1), :] for j in range(group)]
        index = jnp.concatenate(index, axis=1) if group > 1 else index[0]
        places = lax.broadcasted_iota(jnp.int32, (height, group * samples), 0)
        hot = jnp.where(places == index, 1.0, 0.0).astype(LOW)
        both = jnp.dot(base_ref[...], hot, preferred_element_type=F32).astype(LOW)
        for j in range(group):
            c = i * size + first + j
            columns = slice(j * samples, (j + 1) * samples)
            table = jnp.concatenate([both[:height, columns], both[height:, columns]], axis=1)
            table_ref[c] = table
            real, imag = dual_ref[c, 0], dual_ref[c, 1]
            right = jnp.concatenate(
                [
                    jnp.concatenate([real, -imag], axis=1),
                    jnp.concatenate([imag, real], axis=1),
                ],
                axis=0,
            ).astype(LOW)
            spread = lax.dot_general(
                table, right, (((1,), (1,)), ((), ())), preferred_element_type=F32
            ).astype(LOW)
            hold[first + j] = spread.reshape(n, height // n, 2 * width)
            for d in range(n):
                outs[d][c] = hold[first + j, partner(me, d, n)]


def spread_call(n, height, sample_rows, row_base, dual_data):
    channels, _, width, samples = dual_data.shape
    size = pick(channels, 8)
    block = shape_of((channels, height // n, 2 * width), LOW)
    table = shape_of((channels, height, 2 * samples), LOW)
    return streamed(
        functools.partial(spread_body, n, size),
        (dual_data,),
        (),
        (table,) + (block,) * n,
        channels // size,
        [pltpu.VMEM((size, n, height // n, 2 * width), LOW)],
        soon=(sample_rows, row_base),
        room=False,
    )


TWIST = LOWPASS[1] / LOWPASS[0]
RATIO = LOWPASS[3] / LOWPASS[0]
GAIN = LOWPASS[0] ** 2 / 2.0


def moved(blocks, shift, lane):
    rolled = [pltpu.roll(block, shift % 128, 1) for block in blocks]
    empty = jnp.zeros_like(rolled[0])
    if shift > 0:
        return [jnp.where(lane >= shift, r, p) for r, p in zip(rolled, [empty] + rolled[:-1])]
    return [jnp.where(lane < 128 + shift, r, p) for r, p in zip(rolled, rolled[1:] + [empty])]


def each(function, *lists):
    return [function(*items) for items in zip(*lists)]


def blocks_of(columns):
    return [slice(at, at + 128) for at in range(0, columns, 128)]


def synth_body(size, i, ins, whole, outs, scratch):
    (wave_ref, before_ref, after_ref, image_ref, dual_ref), (out_ref,), (holds,) = ins, outs, scratch
    rows, columns = image_ref.shape[1:]
    blocks = blocks_of(columns)
    lane = lax.broadcasted_iota(jnp.int32, (8, 128), 1)

    for j in range(size):
        c = i * size + j
        hold = holds.at[j]
        for band in range(2):
            for at, block in enumerate(blocks):
                low = wave_ref[c, band, :, block].astype(F32)
                high = wave_ref[c, 2 + band, :, block].astype(F32)
                hold[band, at, 8 : 8 + rows] = low + RATIO * high
                hold[2 + band, at, 8 : 8 + rows] = high - RATIO * low
                low = after_ref[c, band, :, block].astype(F32)
                high = after_ref[c, 2 + band, :, block].astype(F32)
                hold[band, at, 8 + rows : 9 + rows] = low + RATIO * high
                low = before_ref[c, band, :, block].astype(F32)
                high = before_ref[c, 2 + band, :, block].astype(F32)
                hold[2 + band, at, 6:8] = high - RATIO * low
        for start in range(0, rows, 8):
            mixed = [
                [
                    hold[band, at, pl.ds(start + 9, 8)]
                    + TWIST * hold[band, at, pl.ds(start + 8, 8)]
                    + TWIST * hold[2 + band, at, pl.ds(start + 7, 8)]
                    - hold[2 + band, at, pl.ds(start + 6, 8)]
                    for at in range(len(blocks))
                ]
                for band in range(2)
            ]
            straight = each(lambda u, v: u + RATIO * v, *mixed)
            crossed = each(lambda u, v: v - RATIO * u, *mixed)
            crossed = each(lambda u, v: TWIST * u - v, crossed, moved(crossed, 1, lane))
            parts = moved(straight, -1, lane), straight, moved(crossed, 1, lane)
            for block, u, v, w in zip(blocks, *parts):
                own = (c, slice(start, start + 8), block)
                synth = u + TWIST * v + w
                out_ref[own] = image_ref[own] - 0.5 * (GAIN * synth + dual_ref[own])


def synth_call(wave, before, after, image, dual_nuclear):
    channels, rows, columns = image.shape
    size = pick(channels, 4)
    return streamed(
        functools.partial(synth_body, size),
        (wave, before, after, image, dual_nuclear),
        (),
        (shape_of(image.shape, F32),),
        channels // size,
        [pltpu.VMEM((size, 4, columns // 128, rows + 16, 128), F32)],
    )[0]


def image_body(n, size, i, ins, whole, outs, scratch):
    got, (base_ref, image_ref, dual_ref, col_ref) = whole[:n], whole[n:]
    (next_ref, stacked_ref, top_ref, bottom_ref), outs = outs[:4], outs[4:]
    me = position()
    rows, columns = image_ref.shape[1:]
    width = got[0].shape[2]
    tall = size * rows
    own = pl.ds(i * size, size)
    blocks = [got[d][own].reshape(tall, width) for d in range(n)]
    tables = [col_ref[partner(me, d, n)] for d in range(n)]
    if width % 128 == 0:
        back = jnp.dot(
            jnp.concatenate(blocks, axis=1),
            jnp.concatenate(tables, axis=0),
            preferred_element_type=F32,
        )
    else:
        back = sum(
            jnp.dot(block, table, preferred_element_type=F32)
            for block, table in zip(blocks, tables)
        )
    following = jnp.maximum(base_ref[own].reshape(tall, columns) - 0.5 * back, 0.0)
    next_ref[own] = following.reshape(size, rows, columns)
    field = 2.0 * following - image_ref[own].reshape(tall, columns)
    stacked_ref[own] = (dual_ref[own].reshape(tall, columns) + field).astype(LOW).reshape(
        size, rows, columns
    )
    low = field.astype(LOW)
    edges = field.reshape(size, rows, columns)
    top_ref[own] = edges[:, 0:2].astype(LOW)
    bottom_ref[own] = edges[:, rows - 1 : rows].astype(LOW)
    form = (((1,), (1,)), ((), ()))
    if width % 128 == 0:
        spectra = lax.dot_general(
            low, jnp.concatenate(tables, axis=0), form, preferred_element_type=F32
        ).astype(LOW)
        parts = [spectra[:, d * width : (d + 1) * width] for d in range(n)]
    else:
        parts = [
            lax.dot_general(low, table, form, preferred_element_type=F32).astype(LOW)
            for table in tables
        ]
    for d in range(n):
        outs[d][own] = parts[d].reshape(size, rows, width)


def image_call(n, got, col_table, base, image, dual_nuclear):
    channels, _, columns = image.shape
    size = pick(channels, 8)
    outs = (
        shape_of(image.shape, F32),
        shape_of(image.shape, LOW),
        shape_of((channels, 2, columns), LOW),
        shape_of((channels, 1, columns), LOW),
    ) + tuple(shape_of(g.shape, LOW) for g in got)
    return streamed(
        functools.partial(image_body, n, size),
        (),
        tuple(got) + (base, image, dual_nuclear, col_table),
        outs,
        channels // size,
    )


def sample_body(n, size, i, ins, whole, outs, scratch):
    got, (table_ref, dual_ref, seen_ref), (out_ref,), (hold,) = whole[:n], whole[n:], outs, scratch
    me = position()
    height, pairs = table_ref.shape[1:]
    samples = pairs // 2
    width = dual_ref.shape[2]
    for j in range(size):
        c = i * size + j
        for d in range(n):
            hold[j, partner(me, d, n)] = got[d][c]
        product = lax.dot_general(
            hold[j].reshape(height, 2 * width),
            table_ref[c],
            (((0,), (0,)), ((), ())),
            preferred_element_type=F32,
        )
        real = product[:width, :samples] + product[width:, samples:]
        imag = product[width:, :samples] - product[:width, samples:]
        for part, value in ((0, real), (1, imag)):
            out_ref[c, part] = (dual_ref[c, part] + 0.5 * (value - seen_ref[c, part])) / 1.5


def sample_call(n, got, table, dual_data, observed, earlier):
    channels, _, width, _ = dual_data.shape
    height = table.shape[1]
    size = pick(channels, 4)
    return streamed(
        functools.partial(sample_body, n, size),
        (),
        tuple(got) + (table, dual_data, observed),
        (shape_of(dual_data.shape, F32),),
        channels // size,
        [pltpu.VMEM((size, n, height // n, 2 * width), LOW)],
        earlier,
    )[0]


def bands_body(size, final, i, ins, whole, outs, scratch):
    next_ref, image_ref, wave_ref, before_ref, after_ref = ins
    holds, edges, scale = scratch
    rows, columns = image_ref.shape[1:]
    blocks = blocks_of(columns)
    lane = lax.broadcasted_iota(jnp.int32, (8, 128), 1)
    half = 0.5 * GAIN

    @pl.when(i == 0)
    def _():
        if final:
            limit = 0.6 * math.sqrt(CH)
            scale[...] = 1.0 / jnp.maximum(1.0, jnp.sqrt(whole[0][...]) / limit)
        else:
            scale[...] = jnp.zeros_like(scale)
        edges[...] = jnp.zeros_like(edges)

    def filtered(field):
        back, ahead, far = (moved(field, shift, lane) for shift in (1, -1, -2))
        early = each(lambda u, v: u + TWIST * v, back, field)
        late = each(lambda u, v: TWIST * u - v, ahead, far)
        low = each(lambda u, v: u - RATIO * v, early, late)
        high = each(lambda u, v: RATIO * u + v, early, late)
        return low, high

    def one(j, _):
        c = i * size + j
        edges[0:1] = half * before_ref[c].astype(F32)
        edges[1:3] = half * after_ref[c].astype(F32)
        for band, parts in enumerate(filtered([edges[:, block] for block in blocks])):
            for at, part in enumerate(parts):
                holds[band, at, 7:8] = part[0:1]
                holds[band, at, 8 + rows : 10 + rows] = part[1:3]
        for start in range(0, rows, 8):
            own = slice(start, start + 8)
            field = [
                GAIN * next_ref[c, own, block] - half * image_ref[c, own, block]
                for block in blocks
            ]
            for band, parts in enumerate(filtered(field)):
                for at, part in enumerate(parts):
                    holds[band, at, 8 + start : 16 + start] = part
        for start in range(0, rows, 16):
            for at, block in enumerate(blocks):
                for col_band in range(2):
                    halves = []
                    for piece in (start, start + 8):
                        near = [holds[col_band, at, pl.ds(piece + 7 + k, 8)] for k in range(4)]
                        early = near[0] + TWIST * near[1]
                        late = TWIST * near[2] - near[3]
                        halves.append((early - RATIO * late, RATIO * early + late))
                    for row_band in range(2):
                        band = 2 * row_band + col_band
                        both = jnp.concatenate([h[row_band] for h in halves], axis=0)
                        own = (slice(start, start + 16), block)
                        value = wave_ref[(c, band) + own].astype(F32) + both
                        if final:
                            outs[0][(c, band) + own] = (value * scale[(band,) + own]).astype(LOW)
                        else:
                            scale[(band,) + own] += value * value
        return 0

    lax.fori_loop(0, size, one, 0, unroll=size)


def power_late(outs, scratch):
    outs[0][...] = scratch[2][...].astype(LOW)


def bands_call(following, image, wave, before, after, power=None):
    channels, rows, columns = image.shape
    size = pick(channels, 4)
    final = power is not None
    args = (following, image, wave, before, after)
    out = shape_of(wave.shape if final else (4, rows, columns), LOW)
    return streamed(
        functools.partial(bands_body, size, final),
        args,
        (power,) if final else (),
        (out,),
        channels // size,
        [
            pltpu.VMEM((2, columns // 128, rows + 16, 128), F32),
            pltpu.VMEM((8, columns), F32),
            pltpu.VMEM((4, rows, columns), F32),
        ],
        late=None if final else power_late,
    )[0]


def polar_mixing(gram, pixels):
    trace_sum = jnp.trace(gram)
    approx = 2.0 / trace_sum * gram
    eye_mat = jnp.eye(gram.shape[0], dtype=jnp.float32)
    root = eye_mat
    for _ in range(NS_STEPS):
        newton = 1.5 * eye_mat - 0.5 * jnp.dot(root, approx, precision=HIGH)
        approx = jnp.dot(approx, newton, precision=HIGH)
        root = jnp.dot(newton, root, precision=HIGH)
    return (root.astype(LOW), jnp.sqrt(2.0 * pixels / trace_sum))


def rotated(values, axis, shift):
    count = lax.axis_size(axis)
    return lax.ppermute(values, axis, [(i, (i + shift) % count) for i in range(count)])


def sending_order(n):
    half, quarter = n // 2, n // 4
    return [
        *range(half, half + quarter),
        *range(2, half),
        *range(max(half + quarter, 2), n),
        *([1] if n > 1 else []),
    ]


def exchanged(blocks):
    n = len(blocks)
    got = list(blocks)
    for d in sending_order(n):
        got[d] = lax.ppermute(blocks[d], LINE, [(i, partner(i, d, n)) for i in range(n)])
    return got


def neighbours(first, last):
    count = lax.axis_size(LINE)
    up = [(i, i + 1) for i in range(count - 1)]
    down = [(j, i) for i, j in up]
    before = lax.ppermute(last, LINE, up)
    after = lax.ppermute(first, LINE, down)
    return before, after


def total(values, axis):
    result = values.astype(F32)
    for d in range(1, lax.axis_size(axis)):
        result = result + rotated(values, axis, d).astype(F32)
    return result


def shards(image, dual_nuclear, dual_wavelet, dual_data, observed, sample_rows):
    channels, row_count, columns = image.shape
    halves = lax.axis_size("sub")
    n = lax.axis_size("facet") * halves
    height = row_count * n
    width = columns // n
    row_base = jnp.asarray(np.concatenate(host_tables(height), axis=0))
    col_cos, col_sin = host_tables(columns)
    col_table = jnp.asarray(
        np.concatenate(
            [
                col_cos.reshape(n, width, columns),
                (-col_sin.astype(np.float32)).astype(LOW).reshape(n, width, columns),
            ],
            axis=1,
        )
    )

    table, *spread = spread_call(n, height, sample_rows, row_base, dual_data)
    pieces = exchanged(spread)
    cut_wavelet, _ = lax.optimization_barrier((dual_wavelet, spread[-1]))
    edges = (cut_wavelet[:, :, :1], cut_wavelet[:, :, row_count - 2 :])
    wave_before, wave_after = neighbours(*edges)
    base = synth_call(dual_wavelet, wave_before, wave_after, image, dual_nuclear)
    image_next, stacked, top, bottom, *spectra = image_call(
        n, pieces, col_table, base, image, dual_nuclear
    )
    gathered = exchanged(spectra)
    z_before, z_after = neighbours(top, bottom)
    whole = [stacked]
    for d in range(1, lax.axis_size("chan")):
        whole.append(rotated(stacked, "chan", d))
    power = bands_call(image_next, image, dual_wavelet, z_before, z_after)
    power = total(power, "chan")
    wavelet_next = bands_call(image_next, image, dual_wavelet, z_before, z_after, power)

    whole = jnp.concatenate([w.reshape(channels, -1) for w in whole], axis=0)
    gram = jnp.dot(whole, whole.T, preferred_element_type=F32)
    gram = total(gram, "sub")
    mixing, factor = polar_mixing(gram, row_count * columns * halves)
    nuclear_next = factor * jnp.dot(mixing[:channels], whole, preferred_element_type=F32)
    nuclear_next = nuclear_next.reshape(channels, row_count, columns)

    data_next = sample_call(
        n, gathered, table, dual_data, observed, (wavelet_next, nuclear_next)
    )
    return (image_next, nuclear_next, wavelet_next, data_next)


def solution(mesh):
    placed = (
        P(("cube", "chan"), ("facet", "sub"), None),
        P(("cube", "chan"), ("facet", "sub"), None),
        P(("cube", "chan"), None, ("facet", "sub"), None),
        P(("cube", "chan"), None, ("facet", "sub"), None),
        P(("cube", "chan"), None, ("facet", "sub"), None),
        P(("cube", "chan"), None),
    )

    return jax.shard_map(
        shards,
        mesh=mesh,
        in_specs=placed,
        out_specs=(
            P(("cube", "chan"), ("facet", "sub"), None),
            P(("cube", "chan"), ("facet", "sub"), None),
            P(("cube", "chan"), None, ("facet", "sub"), None),
            P(("cube", "chan"), None, ("facet", "sub"), None),
        ),
        check_vma=False,
    )
```

```python
import functools
import math

import jax
import jax.numpy as jnp
import numpy as np
from jax import lax
from jax.experimental import pallas as pl
from jax.experimental.pallas import tpu as pltpu
from jax.sharding import PartitionSpec as P


CH = 64
NS_STEPS = 6


LOWPASS = [0.48296291314453416, 0.8365163037378079, 0.2241438680420134, -0.12940952255126037]
HIGH = lax.Precision.HIGHEST
LOW = jnp.bfloat16
F32 = jnp.float32
LINE = ("facet", "sub")
MIB = 1 << 20
PARTS = 2
BAND = jnp.bfloat16


def host_tables(period):
    index = np.arange(period)
    product = np.outer(index, index) % period
    angles = np.float32(2.0 * math.pi / period) * product.astype(np.float32)
    norm = np.float32(1.0 / math.sqrt(period))
    cos = (np.cos(angles).astype(np.float32) * norm).astype(LOW)
    sin = (np.sin(angles).astype(np.float32) * norm).astype(LOW)
    return cos, sin


def position():
    return lax.axis_index("facet") * lax.axis_size("sub") + lax.axis_index("sub")


def partner(me, d, n):
    assert n & (n - 1) == 0
    return me ^ d


def pick(channels, most):
    size = most
    while channels % size:
        size //= 2
    return size


def nbytes(array):
    return math.prod(array.shape) * jnp.dtype(array.dtype).itemsize


def streamed(
    body,
    ins,
    whole,
    outs,
    chunks,
    part=None,
    scratch=(),
    earlier=(),
    late=None,
    soon=(),
    room=True,
    into=None,
):
    first, count = part or (0, 0)
    sizes = [count or a.shape[0] for a in ins], [count or a.shape[0] for a in outs]
    starts = [
        [first if a.shape[0] > size else 0 for a, size in zip(arrays, lengths)]
        for arrays, lengths in zip((ins, outs), sizes)
    ]
    into = into or [None] * len(outs)
    held = [a for a in into if a is not None]
    chunked = range(len(outs) - (late is not None))

    def kernel(*refs):
        refs = list(refs)
        take = lambda many: [refs.pop(0) for _ in range(many)]
        in_far, whole_near, _ = take(len(ins)), take(len(whole)), take(len(earlier))
        soon_far, _ = take(len(soon)), take(len(held))
        out_far, in_near, out_near = take(len(outs)), take(len(ins)), take(len(outs))
        extra, soon_near = take(len(scratch)), take(len(soon))
        in_sem, out_sem, soon_sem = refs
        firsts = [
            pltpu.make_async_copy(soon_far[a], soon_near[a], soon_sem.at[a])
            for a in range(len(soon))
        ]

        def arrival(a, i):
            step = sizes[0][a] // chunks
            return pltpu.make_async_copy(
                in_far[a].at[pl.ds(starts[0][a] + i * step, step)],
                in_near[a].at[pl.ds(i * step, step)],
                in_sem.at[a, i],
            )

        def departure(a, i):
            step = sizes[1][a] // chunks
            return pltpu.make_async_copy(
                out_near[a].at[pl.ds(i * step, step)],
                out_far[a].at[pl.ds(starts[1][a] + i * step, step)],
                out_sem.at[a, i],
            )

        for copy in firsts:
            copy.start()

        @pl.loop(0, chunks)
        def _(i):
            for a in range(len(ins)):
                arrival(a, i).start()

        for copy in firsts:
            copy.wait()

        @pl.loop(0, chunks)
        def _(i):
            for a in range(len(ins)):
                arrival(a, i).wait()
            body(i, in_near, whole_near + soon_near, out_near, extra)
            for a in chunked:
                departure(a, i).start()

        if late is not None:
            late(out_near, extra)
            last = len(outs) - 1
            copy = pltpu.make_async_copy(out_near[last], out_far[last], out_sem.at[last, 0])
            copy.start()
            copy.wait()

        @pl.loop(0, chunks)
        def _(i):
            for a in chunked:
                departure(a, i).wait()

    far = pl.BlockSpec(memory_space=pltpu.HBM)
    anywhere = pl.BlockSpec(memory_space=pl.ANY)
    near = pl.BlockSpec(memory_space=pltpu.VMEM)
    buffers = [
        pltpu.VMEM((size,) + a.shape[1:], a.dtype)
        for arrays, lengths in zip((ins, outs), sizes)
        for a, size in zip(arrays, lengths)
    ]
    taken = buffers + list(scratch) + list(soon)
    moved_bytes = sum(nbytes(a) for a in list(ins) + list(outs) + list(whole))
    operands = (*ins, *whole, *earlier, *soon, *held)
    at = len(operands) - len(held)
    aliases = {}
    for index, array in enumerate(into):
        if array is not None:
            aliases[at + len(aliases)] = index
    return pl.pallas_call(
        kernel,
        out_shape=tuple(outs),
        in_specs=[far] * len(ins)
        + [near] * len(whole)
        + [anywhere] * len(earlier)
        + [far] * (len(soon) + len(held)),
        out_specs=(far,) * len(outs),
        input_output_aliases=aliases,
        scratch_shapes=buffers
        + list(scratch)
        + [pltpu.VMEM(a.shape, a.dtype) for a in soon]
        + [
            pltpu.SemaphoreType.DMA((max(len(ins), 1), chunks)),
            pltpu.SemaphoreType.DMA((len(outs), chunks)),
            pltpu.SemaphoreType.DMA((max(len(soon), 1),)),
        ],
        compiler_params=pltpu.CompilerParams(
            vmem_limit_bytes=sum(nbytes(a) for a in taken) + 4 * MIB if room else None
        ),
        cost_estimate=pl.CostEstimate(
            flops=4 * 10**9, bytes_accessed=moved_bytes, transcendentals=0
        ),
    )(*operands)


def shape_of(shape, dtype):
    return jax.ShapeDtypeStruct(shape, dtype)


def spread_body(n, size, start, i, ins, whole, outs, scratch):
    (dual_ref,), (rows_ref, base_ref), (table_ref, *outs), (hold,) = ins, whole, outs, scratch
    me = position()
    height = table_ref.shape[1]
    samples = rows_ref.shape[1]
    width = dual_ref.shape[2]
    group = 2 if size % 2 == 0 else 1
    for first in range(0, size, group):
        index = [rows_ref[pl.ds(start + i * size + first + j, 1), :] for j in range(group)]
        index = jnp.concatenate(index, axis=1) if group > 1 else index[0]
        places = lax.broadcasted_iota(jnp.int32, (height, group * samples), 0)
        hot = jnp.where(places == index, 1.0, 0.0).astype(LOW)
        both = jnp.dot(base_ref[...], hot, preferred_element_type=F32).astype(LOW)
        for j in range(group):
            c = i * size + first + j
            columns = slice(j * samples, (j + 1) * samples)
            table = jnp.concatenate([both[:height, columns], both[height:, columns]], axis=1)
            table_ref[c] = table
            real, imag = dual_ref[c, 0], dual_ref[c, 1]
            right = jnp.concatenate(
                [
                    jnp.concatenate([real, -imag], axis=1),
                    jnp.concatenate([imag, real], axis=1),
                ],
                axis=0,
            ).astype(LOW)
            spread = lax.dot_general(
                table, right, (((1,), (1,)), ((), ())), preferred_element_type=F32
            ).astype(LOW)
            hold[first + j] = spread.reshape(n, height // n, 2 * width)
            for d in range(n):
                outs[d][c] = hold[first + j, partner(me, d, n)]


def spread_call(n, height, sample_rows, row_base, dual_data, part):
    _, _, width, samples = dual_data.shape
    channels = part[1]
    size = pick(channels, 8)
    block = shape_of((channels, height // n, 2 * width), LOW)
    table = shape_of((channels, height, 2 * samples), LOW)
    return streamed(
        functools.partial(spread_body, n, size, part[0]),
        (dual_data,),
        (),
        (table,) + (block,) * n,
        channels // size,
        part,
        [pltpu.VMEM((size, n, height // n, 2 * width), LOW)],
        soon=(sample_rows, row_base),
        room=part[0] > 0,
    )


TWIST = LOWPASS[1] / LOWPASS[0]
RATIO = LOWPASS[3] / LOWPASS[0]
GAIN = LOWPASS[0] ** 2 / 2.0


def moved(blocks, shift, lane):
    rolled = [pltpu.roll(block, shift % 128, 1) for block in blocks]
    empty = jnp.zeros_like(rolled[0])
    if shift > 0:
        return [jnp.where(lane >= shift, r, p) for r, p in zip(rolled, [empty] + rolled[:-1])]
    return [jnp.where(lane < 128 + shift, r, p) for r, p in zip(rolled, rolled[1:] + [empty])]


def each(function, *lists):
    return [function(*items) for items in zip(*lists)]


def blocks_of(columns):
    return [slice(at, at + 128) for at in range(0, columns, 128)]


def synth_body(size, i, ins, whole, outs, scratch):
    (wave_ref, before_ref, after_ref, image_ref, dual_ref), (out_ref,), (holds,) = ins, outs, scratch
    rows, columns = image_ref.shape[1:]
    blocks = blocks_of(columns)
    lane = lax.broadcasted_iota(jnp.int32, (8, 128), 1)

    for j in range(size):
        c = i * size + j
        hold = holds.at[j]
        for band in range(2):
            for at, block in enumerate(blocks):
                low = wave_ref[c, band, :, block].astype(F32)
                high = wave_ref[c, 2 + band, :, block].astype(F32)
                hold[band, at, 8 : 8 + rows] = low + RATIO * high
                hold[2 + band, at, 8 : 8 + rows] = high - RATIO * low
                low = after_ref[c, band, :, block].astype(F32)
                high = after_ref[c, 2 + band, :, block].astype(F32)
                hold[band, at, 8 + rows : 9 + rows] = low + RATIO * high
                low = before_ref[c, band, :, block].astype(F32)
                high = before_ref[c, 2 + band, :, block].astype(F32)
                hold[2 + band, at, 6:8] = high - RATIO * low
        for start in range(0, rows, 8):
            mixed = [
                [
                    hold[band, at, pl.ds(start + 9, 8)]
                    + TWIST * hold[band, at, pl.ds(start + 8, 8)]
                    + TWIST * hold[2 + band, at, pl.ds(start + 7, 8)]
                    - hold[2 + band, at, pl.ds(start + 6, 8)]
                    for at in range(len(blocks))
                ]
                for band in range(2)
            ]
            straight = each(lambda u, v: u + RATIO * v, *mixed)
            crossed = each(lambda u, v: v - RATIO * u, *mixed)
            crossed = each(lambda u, v: TWIST * u - v, crossed, moved(crossed, 1, lane))
            parts = moved(straight, -1, lane), straight, moved(crossed, 1, lane)
            for block, u, v, w in zip(blocks, *parts):
                own = (c, slice(start, start + 8), block)
                synth = u + TWIST * v + w
                out_ref[own] = image_ref[own] - 0.5 * (GAIN * synth + dual_ref[own])


def synth_call(wave, before, after, image, dual_nuclear):
    channels, rows, columns = image.shape
    size = pick(channels, 4)
    return streamed(
        functools.partial(synth_body, size),
        (wave, before, after, image, dual_nuclear),
        (),
        (shape_of(image.shape, F32),),
        channels // size,
        scratch=[pltpu.VMEM((size, 4, columns // 128, rows + 16, 128), F32)],
    )[0]


def image_body(n, size, start, i, ins, whole, outs, scratch):
    got, (base_ref, image_ref, dual_ref, col_ref) = whole[:n], whole[n:]
    (next_ref, stacked_ref, edge_ref), outs = outs[:3], outs[3:]
    me = position()
    rows, columns = image_ref.shape[1:]
    width = got[0].shape[2]
    tall = size * rows
    own, here = pl.ds(i * size, size), pl.ds(start + i * size, size)
    blocks = [got[d][own].reshape(tall, width) for d in range(n)]
    tables = [col_ref[partner(me, d, n)] for d in range(n)]
    if width % 128 == 0:
        back = jnp.dot(
            jnp.concatenate(blocks, axis=1),
            jnp.concatenate(tables, axis=0),
            preferred_element_type=F32,
        )
    else:
        back = sum(
            jnp.dot(block, table, preferred_element_type=F32)
            for block, table in zip(blocks, tables)
        )
    following = jnp.maximum(base_ref[here].reshape(tall, columns) - 0.5 * back, 0.0)
    next_ref[own] = following.reshape(size, rows, columns)
    field = 2.0 * following - image_ref[here].reshape(tall, columns)
    stacked_ref[own] = (dual_ref[here].reshape(tall, columns) + field).astype(LOW).reshape(
        size, rows, columns
    )
    low = field.astype(LOW)
    edges = field.reshape(size, rows, columns)
    edge_ref[own, 0:2] = edges[:, 0:2].astype(LOW)
    edge_ref[own, 2:3] = edges[:, rows - 1 : rows].astype(LOW)
    form = (((1,), (1,)), ((), ()))
    if width % 128 == 0:
        spectra = lax.dot_general(
            low, jnp.concatenate(tables, axis=0), form, preferred_element_type=F32
        ).astype(LOW)
        parts = [spectra[:, d * width : (d + 1) * width] for d in range(n)]
    else:
        parts = [
            lax.dot_general(low, table, form, preferred_element_type=F32).astype(LOW)
            for table in tables
        ]
    for d in range(n):
        outs[d][own] = parts[d].reshape(size, rows, width)


def image_call(n, got, col_table, base, image, dual_nuclear, part, into):
    channels, _, columns = image.shape
    size = pick(part[1], 8)
    outs = (
        shape_of(image.shape, F32),
        shape_of((part[1],) + image.shape[1:], LOW),
        shape_of((channels, 3, columns), LOW),
    ) + tuple(shape_of(g.shape, LOW) for g in got)
    return streamed(
        functools.partial(image_body, n, size, part[0]),
        (),
        tuple(got) + (base, image, dual_nuclear, col_table),
        outs,
        part[1] // size,
        part,
        into=into and into + [None] * n,
    )


def sample_body(n, size, start, i, ins, whole, outs, scratch):
    got, (table_ref, dual_ref, seen_ref), (out_ref,), (hold,) = whole[:n], whole[n:], outs, scratch
    me = position()
    height, pairs = table_ref.shape[1:]
    samples = pairs // 2
    width = dual_ref.shape[2]
    for j in range(size):
        c = i * size + j
        for d in range(n):
            hold[j, partner(me, d, n)] = got[d][c]
        product = lax.dot_general(
            hold[j].reshape(height, 2 * width),
            table_ref[c],
            (((0,), (0,)), ((), ())),
            preferred_element_type=F32,
        )
        real = product[:width, :samples] + product[width:, samples:]
        imag = product[width:, :samples] - product[:width, samples:]
        for part, value in ((0, real), (1, imag)):
            out_ref[c, part] = (
                dual_ref[start + c, part] + 0.5 * (value - seen_ref[start + c, part])
            ) / 1.5


def sample_call(n, got, table, dual_data, observed, earlier, part, into):
    width = dual_data.shape[2]
    height = table.shape[1]
    size = pick(part[1], 4)
    return streamed(
        functools.partial(sample_body, n, size, part[0]),
        (),
        tuple(got) + (table, dual_data, observed),
        (shape_of(dual_data.shape, F32),),
        part[1] // size,
        part,
        [pltpu.VMEM((size, n, height // n, 2 * width), LOW)],
        earlier,
        into=into,
    )[0]


def power_body(size, i, ins, whole, outs, scratch):
    next_ref, image_ref, wave_ref, even_ref, odd_ref = ins
    first_of_pair = lax.rem(position(), 2) == 0
    holds, edges, scale = scratch
    rows, columns = image_ref.shape[1:]
    blocks = blocks_of(columns)
    lane = lax.broadcasted_iota(jnp.int32, (8, 128), 1)
    half = 0.5 * GAIN

    @pl.when(i == 0)
    def _():
        scale[...] = jnp.zeros_like(scale)
        edges[...] = jnp.zeros_like(edges)

    def filtered(field):
        back, ahead, far = (moved(field, shift, lane) for shift in (1, -1, -2))
        early = each(lambda u, v: u + TWIST * v, back, field)
        late = each(lambda u, v: TWIST * u - v, ahead, far)
        low = each(lambda u, v: u - RATIO * v, early, late)
        high = each(lambda u, v: RATIO * u + v, early, late)
        return low, high

    def one(j, _):
        c = i * size + j
        even, odd = half * even_ref[c].astype(F32), half * odd_ref[c].astype(F32)
        edges[0:3] = jnp.where(first_of_pair, even, odd)
        edges[3:6] = jnp.where(first_of_pair, odd, even)
        for band, parts in enumerate(filtered([edges[:, block] for block in blocks])):
            for at, part in enumerate(parts):
                holds[band, at, 7:8] = part[5:6]
                holds[band, at, 8 + rows : 10 + rows] = part[0:2]
        for start in range(0, rows, 8):
            own = slice(start, start + 8)
            field = [
                GAIN * next_ref[c, own, block] - half * image_ref[c, own, block]
                for block in blocks
            ]
            for band, parts in enumerate(filtered(field)):
                for at, part in enumerate(parts):
                    holds[band, at, 8 + start : 16 + start] = part
        for start in range(0, rows, 16):
            for at, block in enumerate(blocks):
                for col_band in range(2):
                    halves = []
                    for piece in (start, start + 8):
                        near = [holds[col_band, at, pl.ds(piece + 7 + k, 8)] for k in range(4)]
                        early = near[0] + TWIST * near[1]
                        late = TWIST * near[2] - near[3]
                        halves.append((early - RATIO * late, RATIO * early + late))
                    for row_band in range(2):
                        band = 2 * row_band + col_band
                        both = jnp.concatenate([h[row_band] for h in halves], axis=0)
                        own = (slice(start, start + 16), block)
                        value = wave_ref[(c, band) + own].astype(F32) + both
                        outs[0][(c, band) + own] = value.astype(BAND)
                        scale[(band,) + own] += value * value
        return 0

    lax.fori_loop(0, size, one, 0, unroll=size)


def power_late(outs, scratch):
    outs[1][...] = scratch[2][...].astype(LOW)


def power_call(following, image, wave, even, odd, earlier):
    channels, rows, columns = image.shape
    size = pick(channels, 4)
    bands, power = streamed(
        functools.partial(power_body, size),
        (following, image, wave, even, odd),
        (),
        (shape_of(wave.shape, BAND), shape_of((4, rows, columns), LOW)),
        channels // size,
        scratch=[
            pltpu.VMEM((2, columns // 128, rows + 16, 128), F32),
            pltpu.VMEM((8, columns), F32),
            pltpu.VMEM((4, rows, columns), F32),
        ],
        earlier=earlier,
        late=power_late,
    )
    return power, bands


def result_body(size, i, ins, whole, outs, scratch):
    (bands_ref,), (power_ref,), (out_ref,), (scale,) = ins, whole, outs, scratch

    @pl.when(i == 0)
    def _():
        limit = 0.6 * math.sqrt(CH)
        scale[...] = 1.0 / jnp.maximum(1.0, jnp.sqrt(power_ref[...]) / limit)

    for j in range(size):
        c = i * size + j
        out_ref[c] = (bands_ref[c].astype(F32) * scale[...]).astype(LOW)


def result_call(bands, power):
    channels = bands.shape[0]
    size = pick(channels, 4)
    return streamed(
        functools.partial(result_body, size),
        (bands,),
        (power,),
        (shape_of(bands.shape, LOW),),
        channels // size,
        scratch=[pltpu.VMEM(power.shape, F32)],
    )[0]


def polar_kernel(pixels, *refs):
    grams, (root_ref, factor_ref) = refs[:-2], refs[-2:]
    gram = grams[0][...]
    for other in grams[1:]:
        gram = gram + other[...]
    size = gram.shape[0]
    eye_mat = (
        lax.broadcasted_iota(jnp.int32, (size, size), 0)
        == lax.broadcasted_iota(jnp.int32, (size, size), 1)
    ).astype(F32)
    trace_sum = jnp.sum(jnp.sum(gram * eye_mat, axis=1, keepdims=True), axis=0, keepdims=True)
    dot = functools.partial(jnp.dot, precision=HIGH, preferred_element_type=F32)
    approx = (2.0 / trace_sum) * gram
    root = eye_mat
    for turn in range(NS_STEPS):
        newton = 1.5 * eye_mat - 0.5 * (dot(root, approx) if turn else approx)
        if turn < NS_STEPS - 1:
            approx = dot(approx, newton)
        root = dot(newton, root) if turn else newton
    root_ref[...] = root[: root_ref.shape[0]].astype(LOW)
    factor_ref[...] = jnp.broadcast_to(jnp.sqrt(2.0 * pixels / trace_sum), factor_ref.shape)


def polar_call(grams, channels, pixels):
    near = pl.BlockSpec(memory_space=pltpu.VMEM)
    root, factor = pl.pallas_call(
        functools.partial(polar_kernel, pixels),
        out_shape=(shape_of((channels, grams[0].shape[0]), LOW), shape_of((8, 128), F32)),
        in_specs=[near] * len(grams),
        out_specs=(near, near),
        compiler_params=pltpu.CompilerParams(vmem_limit_bytes=8 * MIB),
        name="polar",
        cost_estimate=pl.CostEstimate(flops=2 * 10**9, bytes_accessed=10**5, transcendentals=0),
    )(*grams)
    return root, factor[0, 0]


def rotated(values, axis, shift):
    count = lax.axis_size(axis)
    return lax.ppermute(values, axis, [(i, (i + shift) % count) for i in range(count)])


def sending_order(n):
    half, quarter = n // 2, n // 4
    return [
        *range(half, half + quarter),
        *range(2, half),
        *range(max(half + quarter, 2), n),
        *([1] if n > 1 else []),
    ]


def exchanged(blocks):
    n = len(blocks)
    got = list(blocks)
    for d in sending_order(n):
        got[d] = lax.ppermute(blocks[d], LINE, [(i, partner(i, d, n)) for i in range(n)])
    return got


def neighbours(first, last):
    count = lax.axis_size(LINE)
    up = [(i, i + 1) for i in range(count - 1)]
    down = [(j, i) for i, j in up]
    before = lax.ppermute(last, LINE, up)
    after = lax.ppermute(first, LINE, down)
    return before, after


def total(values, axis):
    result = values.astype(F32)
    for d in range(1, lax.axis_size(axis)):
        result = result + rotated(values, axis, d).astype(F32)
    return result


def shards(image, dual_nuclear, dual_wavelet, dual_data, observed, sample_rows):
    channels, row_count, columns = image.shape
    halves = lax.axis_size("sub")
    n = lax.axis_size("facet") * halves
    height = row_count * n
    width = columns // n
    row_base = jnp.asarray(np.concatenate(host_tables(height), axis=0))
    col_cos, col_sin = host_tables(columns)
    col_table = jnp.asarray(
        np.concatenate(
            [
                col_cos.reshape(n, width, columns),
                (-col_sin.astype(np.float32)).astype(LOW).reshape(n, width, columns),
            ],
            axis=1,
        )
    )

    parts = parts_of(channels)
    tables, pieces = [], []
    for g, part in enumerate(parts):
        table, *spread = spread_call(n, height, sample_rows, row_base, dual_data, part)
        tables.append(table)
        pieces.append(exchanged(spread))
        if g == 0:
            cut_wavelet, _ = lax.optimization_barrier((dual_wavelet, spread[-1]))
            edges = (cut_wavelet[:, :, :1], cut_wavelet[:, :, row_count - 2 :])
            wave_before, wave_after = neighbours(*edges)
    base = synth_call(dual_wavelet, wave_before, wave_after, image, dual_nuclear)
    into, own, gathered = None, [], []
    for g, part in enumerate(parts):
        image_next, stacked, border, *spectra = image_call(
            n, pieces[g], col_table, base, image, dual_nuclear, part, into
        )
        into = [image_next, None, border]
        own.append(stacked)
        gathered.append(exchanged(spectra))
    sides = []
    for start in (0, 1):
        pairs = [(i, i + 1) for i in range(start, n - 1, 2)]
        sides.append(lax.ppermute(border, LINE, pairs + [(j, i) for i, j in pairs]))
    whole = list(own)
    for d in range(1, lax.axis_size("chan")):
        for stacked in own:
            whole.append(rotated(stacked, "chan", d))
    whole = jnp.concatenate([w.reshape(w.shape[0], -1) for w in whole], axis=0)
    gram = jnp.dot(whole, whole.T, preferred_element_type=F32)
    grams = [gram] + [rotated(gram, "sub", d) for d in range(1, halves)]
    mixing, factor = polar_call(grams, channels, row_count * columns * halves)
    nuclear_next = factor * jnp.dot(mixing, whole, preferred_element_type=F32)
    nuclear_next = nuclear_next.reshape(channels, row_count, columns)

    power, bands = power_call(
        image_next, image, dual_wavelet, *sides, ()
    )
    power = total(power, "chan")
    wavelet_next = result_call(bands, power)

    data_next = None
    for g, part in enumerate(parts):
        earlier = (nuclear_next,) if g == len(parts) - 1 else ()
        data_next = sample_call(
            n,
            gathered[g],
            tables[g],
            dual_data,
            observed,
            earlier,
            part,
            [data_next] if g else None,
        )
    return (image_next, nuclear_next, wavelet_next, data_next)


def parts_of(channels):
    count = PARTS if channels % (8 * PARTS) == 0 else 1
    return [(g * channels // count, channels // count) for g in range(count)]


def solution(mesh):
    placed = (
        P(("cube", "chan"), ("facet", "sub"), None),
        P(("cube", "chan"), ("facet", "sub"), None),
        P(("cube", "chan"), None, ("facet", "sub"), None),
        P(("cube", "chan"), None, ("facet", "sub"), None),
        P(("cube", "chan"), None, ("facet", "sub"), None),
        P(("cube", "chan"), None),
    )

    return jax.shard_map(
        shards,
        mesh=mesh,
        in_specs=placed,
        out_specs=(
            P(("cube", "chan"), ("facet", "sub"), None),
            P(("cube", "chan"), ("facet", "sub"), None),
            P(("cube", "chan"), None, ("facet", "sub"), None),
            P(("cube", "chan"), None, ("facet", "sub"), None),
        ),
        check_vma=False,
    )
```
